32 devices in a mesh: grp: 2 (over x), seq: 16 (over z, y, core).
Axes of the slice: x: 2, y: 2, z: 4, core: 2. Of those that a mesh axis runs over, the one named last changes fastest.
Arguments:
- queries: bfloat16 [8192, 32, 128], P(('grp', 'seq')), parts along dimension 0, may hold values from -45 to 45
- keys: bfloat16 [8192, 8, 128], P(('grp', 'seq')), parts along dimension 0, may hold values from -6 to 6
- values: bfloat16 [8192, 8, 128], P(('grp', 'seq')), parts along dimension 0, may hold values from -6 to 6
- global_ids: int32 [8], P('grp'), parts along dimension 0, may hold values from 0 to 31, as said below
- doc_lengths: int32 [32], P('grp'), parts along dimension 0, may hold values from 1 to 1024, 4096 in all
Outputs:
- attended: bfloat16 [8192, 32, 128], P(('grp', 'seq')), parts along dimension 0
The draws below stay inside these ranges and needn't reach their ends.
There are 2 independent parts, one for each index of `grp`. The reference program is written for one: setup_inputs(seed, part) draws one part's arguments, and reference() takes and returns one part's arrays. A program takes and returns all parts, laid end to end along the dimension named above; each array names one. Nothing has to cross between parts.
Inputs may be any that keep to these rules, and one draw needn't show every extreme that they name: `global_ids`: 4 distinct block numbers.
All inputs are finite; a program needn't handle non-finite values.
Results may differ from the reference program's by a relative error of at most 0.0065.
Values may be sent and summed in bfloat16 or wider, within the bound.
A program may use at most 64 MiB of HBM per device.

```python
import math
import jax
import jax.numpy as jnp
import numpy as np
from jax import lax

HEADS = 32
KV_HEADS = 8
HEAD_DIM = 128
BLK = 128
WIN = 3
GLOBAL_BLOCKS = 4
NDOC = 16
TOKENS = 4096
NBLK = 32
MOST_DOC = 1024


def key_field(key):
    return jnp.clip(jax.random.normal(jax.random.fold_in(key, 11), (TOKENS, KV_HEADS, HEAD_DIM), jnp.float32), -6.0, 6.0)


def draw_keys(key, part):
    field = key_field(key)
    return field.astype(jnp.bfloat16)


def draw_queries(key, part):
    drawn = jnp.clip(jax.random.normal(jax.random.fold_in(key, 19), (TOKENS, HEADS, HEAD_DIM), jnp.float32), -6.0, 6.0)
    return drawn.astype(jnp.bfloat16)


def draw_global_ids(key, part):
    shuffled = jax.random.permutation(jax.random.fold_in(key, 5), NBLK)
    return shuffled[:GLOBAL_BLOCKS].astype(jnp.int32)


def steps_of(own_key, shape, pieces, smallest, largest):
    def one(axis_at, blocks):
        draws = jax.random.uniform(jax.random.fold_in(jax.random.fold_in(own_key, 6), axis_at), (blocks,), jnp.float32, smallest / len(pieces), largest / len(pieces))
        return jnp.repeat(jnp.exp(draws), shape[axis_at] // blocks).reshape((-1,) + (1,) * (len(shape) - axis_at - 1))

    loudness = one(*pieces[0])
    for cut in pieces[1:]:
        loudness = loudness * one(*cut)
    return loudness


def profile(amount, total, limit, skew):
    portions = [(1 << 20) // math.isqrt(grade ** skew) + 1 for grade in range(2, amount + 1)]
    spare, counts = total - limit - (amount - 1), [1] * (amount - 1)
    while spare > 0:
        free = [i for i in range(amount - 1) if counts[i] < limit]
        whole, budget = sum([portions[i] for i in free]), spare
        for i in free:
            addition = min(limit - counts[i], max(1, budget * portions[i] // whole), spare)
            counts[i] = counts[i] + addition
            spare = spare - addition
    return np.array([limit] + counts)


def ragged_sizes(rng, count, total, bound, slope):
    if count == 2:
        one = jax.random.randint(rng, (), max(1, total - bound), min(bound, total - 1) + 1)
        return jnp.stack([one, total - one])
    lengths = jnp.asarray(profile(count, total, bound, slope), jnp.int32)
    couples = (count - 1) // 2
    donor, sink = lengths[1:1 + 2 * couples:2], lengths[2:2 + 2 * couples:2]
    slack = jnp.minimum(donor - 1, bound - sink)
    passed = jax.random.randint(jax.random.fold_in(rng, 1), (couples,), 0, 1 << 20) % (slack + 1)
    lengths = lengths.at[1:1 + 2 * couples:2].set(donor - passed).at[2:2 + 2 * couples:2].set(sink + passed)
    return lengths[jax.random.permutation(jax.random.fold_in(rng, 2), count)]


def bell_draw(stream_key, dims, width, most, cuts=(), held_as=jnp.bfloat16):
    values = width * jax.random.normal(stream_key, dims, jnp.float32)
    if cuts:
        values = values * steps_of(stream_key, dims, cuts, -0.22, 0.18)
    return jnp.clip(values, -most, most).astype(held_as)


def setup_inputs(seed: int = 0, part: int = 0) -> dict:
    key_list = jax.random.split(jax.random.key(seed), 6)
    part_splits = jax.random.split(jax.random.fold_in(key_list[5], part), 6)
    queries = draw_queries(jax.random.fold_in(jax.random.fold_in(key_list[5], part), 71), part)
    keys = draw_keys(jax.random.fold_in(jax.random.fold_in(key_list[5], part), 71), part)
    values = bell_draw(part_splits[2], (TOKENS, KV_HEADS, HEAD_DIM), 1.0, 6.0, ((0, 16),))
    global_ids = draw_global_ids(jax.random.fold_in(jax.random.fold_in(key_list[5], part), 71), part)
    doc_lengths = ragged_sizes(part_splits[4], NDOC, TOKENS, MOST_DOC, 2).astype(jnp.int32)
    return {"queries": queries, "keys": keys, "values": values, "global_ids": global_ids, "doc_lengths": doc_lengths}


masked_score = -1e+30

def doc_index(positions, doc_ends):
    return lax.optimization_barrier(jnp.sum((positions[:, None] >= doc_ends[None, :]).astype(jnp.int32), axis=1))

def reference(queries, keys, values, global_ids, doc_lengths):
    group_size = HEADS // KV_HEADS
    score_scale = 1.0 / math.sqrt(HEAD_DIM)
    doc_ends = jnp.cumsum(doc_lengths).astype(jnp.int32)
    offsets = jnp.arange(BLK, dtype=jnp.int32)
    padding = jnp.zeros(((WIN - 1) * BLK, KV_HEADS, HEAD_DIM), keys.dtype)
    key_pad = jnp.concatenate([padding, keys], axis=0)
    val_pad = jnp.concatenate([padding, values], axis=0)
    glob_keys = keys.reshape(NBLK, BLK, KV_HEADS, HEAD_DIM)[global_ids].reshape(GLOBAL_BLOCKS * BLK, KV_HEADS, HEAD_DIM)
    glob_vals = values.reshape(NBLK, BLK, KV_HEADS, HEAD_DIM)[global_ids].reshape(GLOBAL_BLOCKS * BLK, KV_HEADS, HEAD_DIM)
    glob_block = jnp.repeat(global_ids, BLK).astype(jnp.int32)
    window_span = jnp.arange(WIN * BLK, dtype=jnp.int32)

    def one_block(block_id):
        first_row = (block_id * BLK).astype(jnp.int32)
        query_pos = first_row + offsets
        query_doc = doc_index(query_pos, doc_ends)
        query_rows = lax.dynamic_slice_in_dim(queries, first_row, BLK, 0).astype(jnp.float32)
        query_rows = query_rows.reshape(BLK, KV_HEADS, group_size, HEAD_DIM)
        win_keys = lax.dynamic_slice_in_dim(key_pad, first_row, WIN * BLK, 0)
        win_vals = lax.dynamic_slice_in_dim(val_pad, first_row, WIN * BLK, 0)
        win_pos = first_row - (WIN - 1) * BLK + window_span
        win_doc = doc_index(win_pos, doc_ends)
        win_ok = (win_pos[None, :] >= 0) & (win_pos[None, :] <= query_pos[:, None]) & (win_doc[None, :] == query_doc[:, None])
        block_gap = block_id - glob_block
        glob_line = jnp.logical_not((block_gap >= 0) & (block_gap < WIN))
        glob_ok = jnp.broadcast_to(glob_line[None, :], (BLK, GLOBAL_BLOCKS * BLK))
        allowed = jnp.concatenate([win_ok, glob_ok], axis=1)
        all_keys = jnp.concatenate([win_keys, glob_keys], axis=0).astype(jnp.float32)
        all_vals = jnp.concatenate([win_vals, glob_vals], axis=0).astype(jnp.float32)
        scores = jnp.einsum('qkgd,tkd->qkgt', query_rows, all_keys, precision=lax.Precision.HIGHEST) * score_scale
        mask_wide = allowed[:, None, None, :]
        scores = jnp.where(mask_wide, scores, masked_score)
        row_peak = lax.optimization_barrier(jnp.max(scores, axis=-1, keepdims=True))
        exp_terms = jnp.where(mask_wide, jnp.exp(scores - row_peak), 0.0)
        denominator = lax.optimization_barrier(jnp.sum(exp_terms, axis=-1))
        weights = lax.optimization_barrier(exp_terms.astype(jnp.bfloat16)).astype(jnp.float32)
        attended = jnp.einsum('qkgt,tkd->qkgd', weights, all_vals, precision=lax.Precision.HIGHEST) / denominator[..., None]
        return attended.astype(jnp.bfloat16).reshape(BLK, HEADS, HEAD_DIM)
    blocks = lax.map(one_block, jnp.arange(NBLK, dtype=jnp.int32))
    return blocks.reshape(TOKENS, HEADS, HEAD_DIM)
```

```python
import functools
import math

import jax
import jax.numpy as jnp
from jax import lax
from jax.experimental import pallas as pl
from jax.experimental.pallas import tpu as pltpu
from jax.sharding import PartitionSpec as P

BLK = 128
WIN = 3

masked_score = -1e30


def shifted(shard, axis, by):
    length = lax.axis_size(axis)
    pairs = [(i, i + by) for i in range(length) if 0 <= i + by < length]
    return lax.ppermute(shard, axis, pairs)


def fill_bias(rank, lens_ref, bias_ref):
    blocks_here, _, span = bias_ref.shape
    for b in range(blocks_here):
        first = (rank * blocks_here + b) * BLK
        query_pos = first + lax.broadcasted_iota(jnp.int32, (BLK, span), 0)
        key_pos = first - (WIN - 1) * BLK + lax.broadcasted_iota(jnp.int32, (BLK, span), 1)

        def step(d, carry):
            end, lowest = carry
            end = end + lens_ref[d]
            return end, jnp.where(query_pos >= end, end, lowest)

        _, lowest = lax.fori_loop(
            0, lens_ref.shape[0], step, (jnp.int32(0), jnp.zeros((BLK, span), jnp.int32))
        )
        seen = (key_pos >= lowest) & (key_pos <= query_pos)
        bias_ref[b] = jnp.where(seen, 0.0, masked_score)


def attn_kernel(ids_ref, lens_ref, q_ref, own_ref, prev_ref, glob_ref, o_ref, bias_ref):
    group_size, tok_rows, head_size = q_ref.shape
    blocks_here = tok_rows // BLK
    rank = lax.axis_index("seq")
    factor = math.log2(math.e) / math.sqrt(head_size)
    rows = group_size * BLK

    @pl.when(pl.program_id(0) == 0)
    def _():
        fill_bias(rank, lens_ref, bias_ref)

    def near(which, b):
        parts = []
        for i in range(blocks_here + b - WIN + 1, blocks_here + b + 1):
            src, j = (prev_ref, i) if i < blocks_here else (own_ref, i - blocks_here)
            parts.append(src[which, 0, j * BLK : (j + 1) * BLK, :])
        return jnp.concatenate(parts, axis=0)

    dims = (((1,), (1,)), ((), ()))
    for b in range(blocks_here):
        q = q_ref[:, b * BLK : (b + 1) * BLK, :].reshape(rows, head_size)
        s_near = lax.dot_general(q, near(0, b), dims, preferred_element_type=jnp.float32)
        s_near = (s_near.reshape(group_size, BLK, WIN * BLK) + bias_ref[b][None]).reshape(
            rows, WIN * BLK
        )
        s_far = lax.dot_general(q, glob_ref[0, 0], dims, preferred_element_type=jnp.float32)
        far = []
        for s in range(ids_ref.shape[0]):
            gap = rank * blocks_here + b - ids_ref[s]
            shift = jnp.where((gap >= 0) & (gap < WIN), masked_score, 0.0)
            far.append(s_far[:, s * BLK : (s + 1) * BLK] + shift)
        scores = jnp.concatenate([s_near] + far, axis=1)
        peak = jnp.max(scores, axis=1, keepdims=True)
        terms = jnp.exp2((scores - peak) * factor)
        total = jnp.sum(terms, axis=1, keepdims=True)
        weights = terms.astype(jnp.bfloat16)
        held = jnp.concatenate([near(1, b), glob_ref[1, 0]], axis=0)
        out = jnp.dot(weights, held, preferred_element_type=jnp.float32) / total
        o_ref[:, b * BLK : (b + 1) * BLK, :] = out.astype(o_ref.dtype).reshape(
            group_size, BLK, head_size
        )


def attention(ids, lens, q, own, prev, glob):
    heads_here, tok_rows, head_size = q.shape
    kv_count = own.shape[1]
    group_size = heads_here // kv_count
    blocks_here = tok_rows // BLK
    smem = pl.BlockSpec(memory_space=pltpu.SMEM)
    q_spec = pl.BlockSpec((group_size, tok_rows, head_size), lambda k: (k, 0, 0))
    keyed = lambda n: pl.BlockSpec((2, 1, n, head_size), lambda k: (0, k, 0, 0))
    return pl.pallas_call(
        attn_kernel,
        grid=(kv_count,),
        out_shape=jax.ShapeDtypeStruct(q.shape, jnp.bfloat16),
        in_specs=[smem, smem, q_spec, keyed(tok_rows), keyed(tok_rows), keyed(glob.shape[2])],
        out_specs=q_spec,
        scratch_shapes=[pltpu.VMEM((blocks_here, BLK, WIN * BLK), jnp.float32)],
    )(ids, lens, q, own, prev, glob)


def per_device(queries, keys, values, global_ids, doc_lengths):
    tok_rows, heads_here, head_size = queries.shape
    kv_count = keys.shape[1]
    blocks_here = tok_rows // BLK
    rank = lax.axis_index("seq")
    own = jnp.stack([keys, values]).transpose(0, 2, 1, 3)
    prev = shifted(own, "seq", 1)
    mine = global_ids // blocks_here == rank
    slots = global_ids % blocks_here
    glob = own.reshape(2, kv_count, blocks_here, BLK, head_size)[:, :, slots]
    lowest = jnp.array(-jnp.inf, jnp.bfloat16)
    glob = jnp.where(mine[None, None, :, None, None], glob, lowest)
    glob = lax.pmax(glob, "seq")
    glob = glob.reshape(2, kv_count, -1, head_size)
    q = queries.transpose(1, 0, 2)
    out = attention(global_ids, doc_lengths, q, own, prev, glob)
    return out.transpose(1, 0, 2)


def solution(mesh):
    tokens = P(("grp", "seq"), None, None)
    return jax.shard_map(
        per_device,
        mesh=mesh,
        in_specs=(tokens, tokens, tokens, P("grp"), P("grp")),
        out_specs=tokens,
        check_vma=False,
    )
```

```python
import functools
import math

import jax
import jax.numpy as jnp
from jax import lax
from jax.experimental import pallas as pl
from jax.experimental.pallas import tpu as pltpu
from jax.sharding import PartitionSpec as P

BLK = 128
WIN = 3

masked_score = -1e30


def fill_bias(rank, lens_ref, bias_ref):
    blocks_here, _, span = bias_ref.shape
    for b in range(blocks_here):
        first = (rank * blocks_here + b) * BLK
        query_pos = first + lax.broadcasted_iota(jnp.int32, (BLK, span), 0)
        key_pos = first - (WIN - 1) * BLK + lax.broadcasted_iota(jnp.int32, (BLK, span), 1)

        def step(d, carry):
            end, lowest = carry
            end = end + lens_ref[d]
            return end, jnp.where(query_pos >= end, end, lowest)

        _, lowest = lax.fori_loop(
            0, lens_ref.shape[0], step, (jnp.int32(0), jnp.zeros((BLK, span), jnp.int32))
        )
        seen = (key_pos >= lowest) & (key_pos <= query_pos)
        bias_ref[b] = jnp.where(seen, 0.0, masked_score)


def attn_kernel(ids_ref, lens_ref, q_ref, own_ref, prev_ref, glob_ref, o_ref, bias_ref):
    group_size, tok_rows, head_size = q_ref.shape
    blocks_here = tok_rows // BLK
    rank = lax.axis_index("seq")
    factor = math.log2(math.e) / math.sqrt(head_size)
    rows = group_size * BLK

    @pl.when(pl.program_id(0) == 0)
    def _():
        fill_bias(rank, lens_ref, bias_ref)

    def near(which, b):
        parts = []
        for i in range(blocks_here + b - WIN + 1, blocks_here + b + 1):
            src, j = (prev_ref, i) if i < blocks_here else (own_ref, i - blocks_here)
            parts.append(src[which, 0, j * BLK : (j + 1) * BLK, :])
        return jnp.concatenate(parts, axis=0)

    dims = (((1,), (1,)), ((), ()))
    for b in range(blocks_here):
        q = q_ref[:, b * BLK : (b + 1) * BLK, :].reshape(rows, head_size)
        s_near = lax.dot_general(q, near(0, b), dims, preferred_element_type=jnp.float32)
        s_near = (s_near.reshape(group_size, BLK, WIN * BLK) + bias_ref[b][None]).reshape(
            rows, WIN * BLK
        )
        s_far = lax.dot_general(q, glob_ref[0, 0], dims, preferred_element_type=jnp.float32)
        far = []
        for s in range(ids_ref.shape[0]):
            gap = rank * blocks_here + b - ids_ref[s]
            shift = jnp.where((gap >= 0) & (gap < WIN), masked_score, 0.0)
            far.append(s_far[:, s * BLK : (s + 1) * BLK] + shift)
        scores = jnp.concatenate([s_near] + far, axis=1)
        peak = jnp.max(scores, axis=1, keepdims=True)
        terms = jnp.exp2((scores - peak) * factor)
        total = jnp.sum(terms, axis=1, keepdims=True)
        weights = terms.astype(jnp.bfloat16)
        held = jnp.concatenate([near(1, b), glob_ref[1, 0]], axis=0)
        out = jnp.dot(weights, held, preferred_element_type=jnp.float32) / total
        o_ref[:, b * BLK : (b + 1) * BLK, :] = out.astype(o_ref.dtype).reshape(
            group_size, BLK, head_size
        )


def attention(ids, lens, q, own, prev, glob):
    heads_here, tok_rows, head_size = q.shape
    kv_count = own.shape[1]
    group_size = heads_here // kv_count
    blocks_here = tok_rows // BLK
    smem = pl.BlockSpec(memory_space=pltpu.SMEM)
    q_spec = pl.BlockSpec((group_size, tok_rows, head_size), lambda k: (k, 0, 0))
    keyed = lambda n: pl.BlockSpec((2, 1, n, head_size), lambda k: (0, k, 0, 0))
    return pl.pallas_call(
        attn_kernel,
        grid=(kv_count,),
        out_shape=jax.ShapeDtypeStruct(q.shape, jnp.bfloat16),
        in_specs=[smem, smem, q_spec, keyed(tok_rows), keyed(tok_rows), keyed(glob.shape[2])],
        out_specs=q_spec,
        scratch_shapes=[pltpu.VMEM((blocks_here, BLK, WIN * BLK), jnp.float32)],
    )(ids, lens, q, own, prev, glob)


def exchange_kernel(n, ids_ref, own_ref, prev_ref, glob_ref, raw_ref, to_sem, from_sem, pass_sem, land_sem, near_sem):
    rank = lax.axis_index("seq")
    blocks_here, parts = own_ref.shape[1], own_ref.shape[2]
    lines = n // 4
    line, low = rank // 4, rank % 4
    pair = line * 4 + (low + 2) % 4
    partner = rank + 1 - 2 * (rank % 2)

    barrier = pltpu.get_barrier_semaphore()

    def greet(i, carry):
        pl.semaphore_signal(
            barrier, inc=1, device_id={"seq": (rank + i) % n}, device_id_type=pl.DeviceIdType.MESH
        )
        return carry

    lax.fori_loop(1, n, greet, 0)
    pl.semaphore_wait(barrier, n - 1)

    def remote(src, dst, send, recv, device):
        return pltpu.make_async_remote_copy(
            src_ref=src,
            dst_ref=dst,
            send_sem=send,
            recv_sem=recv,
            device_id={"seq": device},
            device_id_type=pl.DeviceIdType.MESH,
        )

    def gather(i):
        dest = (rank + i) % n
        return remote(
            own_ref.at[dest // parts, :, dest % parts],
            raw_ref.at[pl.ds(rank * blocks_here, blocks_here)],
            to_sem.at[i],
            from_sem.at[i],
            dest,
        )

    def spread(i, piece, device):
        region = glob_ref.at[piece // parts, :, piece % parts]
        return remote(region, region, pass_sem.at[i], land_sem.at[i], device)

    def loop(low_end, high_end, body):
        def step(i, carry):
            body(i)
            return carry

        lax.fori_loop(low_end, high_end, step, 0)

    near = remote(own_ref, prev_ref, near_sem.at[0], near_sem.at[1], (rank + 1) % n)
    loop(1, n, lambda i: gather(i).start())

    @pl.when(rank < n - 1)
    def _():
        near.start()

    @pl.when(rank == 0)
    def _():
        prev_ref[...] = jnp.zeros_like(prev_ref)

    raw_ref[pl.ds(rank * blocks_here, blocks_here)] = own_ref[rank // parts, :, rank % parts]
    loop(1, n, lambda i: gather(i).wait_recv())
    for s in range(ids_ref.shape[0]):
        glob_ref[rank // parts, s, rank % parts] = raw_ref[ids_ref[s]]

    mine = lambda j: ((line - j + lines) % lines) * 4 + low
    theirs = lambda j: ((line - j + lines) % lines) * 4 + (low + 2) % 4
    ahead = lambda j: ((line + j) % lines) * 4 + low
    along = lambda j: spread(j, rank, ahead(j))
    across = lambda j: spread(lines + j, mine(j), pair)
    over = lambda j: spread(2 * lines + j, mine(j), partner)
    last = lambda j: spread(3 * lines + j, theirs(j), partner)

    loop(1, lines, lambda j: along(j).start())

    def first_turn(j):
        @pl.when(j > 0)
        def _():
            along(j).wait_recv()

        across(j).start()
        over(j).start()

    loop(0, lines, first_turn)

    def second_turn(j):
        across(j).wait_recv()
        last(j).start()

    loop(0, lines, second_turn)

    def final_turn(j):
        over(j).wait_recv()
        last(j).wait_recv()
        across(j).wait_send()
        over(j).wait_send()
        last(j).wait_send()

    loop(0, lines, final_turn)
    loop(1, lines, lambda j: along(j).wait_send())
    loop(1, n, lambda i: gather(i).wait_send())

    @pl.when(rank < n - 1)
    def _():
        near.wait_send()

    @pl.when(rank > 0)
    def _():
        near.wait_recv()


def exchange(ids, own):
    n = lax.axis_size("seq")
    _, kv_count, tok_rows, head_size = own.shape
    sides = 2 * kv_count
    parts = n // sides
    part_rows = BLK // parts
    blocks_here = tok_rows // BLK
    own = own.reshape(sides, blocks_here, parts, part_rows, head_size)
    slots = ids.shape[0]
    vmem = pl.BlockSpec(memory_space=pltpu.VMEM)
    dma = pltpu.SemaphoreType.DMA
    prev, glob = pl.pallas_call(
        functools.partial(exchange_kernel, n),
        out_shape=(
            jax.ShapeDtypeStruct(own.shape, own.dtype),
            jax.ShapeDtypeStruct((sides, slots, parts, part_rows, head_size), own.dtype),
        ),
        in_specs=[pl.BlockSpec(memory_space=pltpu.SMEM), vmem],
        out_specs=(vmem, vmem),
        scratch_shapes=[
            pltpu.VMEM((n * blocks_here, part_rows, head_size), own.dtype),
            dma((n,)),
            dma((n,)),
            dma((n,)),
            dma((n,)),
            dma((2,)),
        ],
        compiler_params=pltpu.CompilerParams(collective_id=0, has_side_effects=True),
    )(ids, own)
    return (
        prev.reshape(2, kv_count, tok_rows, head_size),
        glob.reshape(2, kv_count, slots * BLK, head_size),
    )


def per_device(queries, keys, values, global_ids, doc_lengths):
    own = jnp.stack([keys, values]).transpose(0, 2, 1, 3)
    prev, glob = exchange(global_ids, own)
    q = queries.transpose(1, 0, 2)
    out = attention(global_ids, doc_lengths, q, own, prev, glob)
    return out.transpose(1, 0, 2)


def solution(mesh):
    tokens = P(("grp", "seq"), None, None)
    return jax.shard_map(
        per_device,
        mesh=mesh,
        in_specs=(tokens, tokens, tokens, P("grp"), P("grp")),
        out_specs=tokens,
        check_vma=False,
    )
```

```python
import functools
import math

import jax
import jax.numpy as jnp
from jax import lax
from jax.experimental import pallas as pl
from jax.experimental.pallas import tpu as pltpu
from jax.sharding import PartitionSpec as P

BLK = 128
WIN = 3

masked_score = -1e30


def fill_bias(rank, lens_ref, bias_ref):
    blocks_here, _, span = bias_ref.shape
    for b in range(blocks_here):
        first = (rank * blocks_here + b) * BLK
        query_pos = first + lax.broadcasted_iota(jnp.int32, (BLK, span), 0)
        key_pos = first - (WIN - 1) * BLK + lax.broadcasted_iota(jnp.int32, (BLK, span), 1)

        def step(d, carry):
            end, lowest = carry
            end = end + lens_ref[d]
            return end, jnp.where(query_pos >= end, end, lowest)

        _, lowest = lax.fori_loop(
            0, lens_ref.shape[0], step, (jnp.int32(0), jnp.zeros((BLK, span), jnp.int32))
        )
        seen = (key_pos >= lowest) & (key_pos <= query_pos)
        bias_ref[b] = jnp.where(seen, 0.0, masked_score)


def fused_kernel(
    n,
    ids_ref,
    lens_ref,
    q_ref,
    own_ref,
    o_ref,
    prev_ref,
    glob_ref,
    raw_ref,
    bias_ref,
    peak_ref,
    total_ref,
    sum_ref,
    to_sem,
    from_sem,
    pass_sem,
    land_sem,
    near_sem,
):
    rank = lax.axis_index("seq")
    blocks_here, parts = own_ref.shape[1], own_ref.shape[2]
    lines = n // 4
    line, low = rank // 4, rank % 4
    pair = line * 4 + (low + 2) % 4
    partner = rank + 1 - 2 * (rank % 2)

    barrier = pltpu.get_barrier_semaphore()

    def greet(i, carry):
        pl.semaphore_signal(
            barrier, inc=1, device_id={"seq": (rank + i) % n}, device_id_type=pl.DeviceIdType.MESH
        )
        return carry

    lax.fori_loop(1, n, greet, 0)
    pl.semaphore_wait(barrier, n - 1)

    def remote(src, dst, send, recv, device):
        return pltpu.make_async_remote_copy(
            src_ref=src,
            dst_ref=dst,
            send_sem=send,
            recv_sem=recv,
            device_id={"seq": device},
            device_id_type=pl.DeviceIdType.MESH,
        )

    def gather(i):
        dest = (rank + i) % n
        return remote(
            own_ref.at[dest // parts, :, dest % parts],
            raw_ref.at[pl.ds(rank * blocks_here, blocks_here)],
            to_sem.at[i],
            from_sem.at[i],
            dest,
        )

    def spread(i, piece, device):
        region = glob_ref.at[piece // parts, :, piece % parts]
        return remote(region, region, pass_sem.at[i], land_sem.at[i], device)

    def loop(low_end, high_end, body):
        def step(i, carry):
            body(i)
            return carry

        lax.fori_loop(low_end, high_end, step, 0)

    near = remote(own_ref, prev_ref, near_sem.at[0], near_sem.at[1], (rank + 1) % n)
    loop(1, n, lambda i: gather(i).start())

    kv_count = own_ref.shape[0] // 2
    head_size = own_ref.shape[-1]
    group_size = q_ref.shape[0] // kv_count
    rows = group_size * BLK
    factor = math.log2(math.e) / math.sqrt(head_size)
    dims = (((1,), (1,)), ((), ()))

    def scores_of(k, b, keys):
        q = q_ref[pl.ds(k * group_size, group_size), b * BLK : (b + 1) * BLK, :]
        return lax.dot_general(
            q.reshape(rows, head_size), keys, dims, preferred_element_type=jnp.float32
        )

    def masked(scores, bias):
        wide = scores.reshape(group_size, BLK, scores.shape[1]) + bias[None]
        return wide.reshape(scores.shape)

    def absorb(k, b, scores, held, first=False):
        peak = jnp.max(scores, axis=1, keepdims=True)
        if not first:
            old = peak_ref[k, b]
            peak = jnp.maximum(peak, old)
        terms = jnp.exp2((scores - peak) * factor)
        total = jnp.sum(terms, axis=1, keepdims=True)
        out = jnp.dot(terms.astype(jnp.bfloat16), held, preferred_element_type=jnp.float32)
        if not first:
            fade = jnp.exp2((old - peak) * factor)
            total = total + total_ref[k, b] * fade
            out = out + sum_ref[k, b] * fade
        return peak, total, out

    def keep(k, b, state):
        peak_ref[k, b], total_ref[k, b], sum_ref[k, b] = state

    fill_bias(rank, lens_ref, bias_ref)

    def own_turn(k):
        for b in range(blocks_here):
            first = max(0, b - WIN + 1)
            count = b + 1 - first
            keys = own_ref[k, first : b + 1].reshape(count * BLK, head_size)
            held = own_ref[kv_count + k, first : b + 1].reshape(count * BLK, head_size)
            scores = masked(scores_of(k, b, keys), bias_ref[b][:, (WIN - count) * BLK :])
            keep(k, b, absorb(k, b, scores, held, first=True))

    loop(0, kv_count, own_turn)

    @pl.when(rank == 0)
    def _():
        prev_ref[...] = jnp.zeros_like(prev_ref)

    raw_ref[pl.ds(rank * blocks_here, blocks_here)] = own_ref[rank // parts, :, rank % parts]
    loop(1, n, lambda i: gather(i).wait_recv())
    for s in range(ids_ref.shape[0]):
        glob_ref[rank // parts, s, rank % parts] = raw_ref[ids_ref[s]]

    mine = lambda j: ((line - j + lines) % lines) * 4 + low
    theirs = lambda j: ((line - j + lines) % lines) * 4 + (low + 2) % 4
    ahead = lambda j: ((line + j) % lines) * 4 + low
    along = lambda j: spread(j, rank, ahead(j))
    across = lambda j: spread(lines + j, mine(j), pair)
    over = lambda j: spread(2 * lines + j, mine(j), partner)
    last = lambda j: spread(3 * lines + j, theirs(j), partner)

    loop(1, lines, lambda j: along(j).start())

    def first_turn(j):
        @pl.when(j > 0)
        def _():
            along(j).wait_recv()

        across(j).start()
        over(j).start()

    loop(0, lines, first_turn)

    def second_turn(j):
        across(j).wait_recv()
        last(j).start()

    loop(0, lines, second_turn)

    def final_turn(j):
        over(j).wait_recv()
        last(j).wait_recv()
        across(j).wait_send()
        over(j).wait_send()
        last(j).wait_send()

    @pl.when(rank < n - 1)
    def _():
        near.start()

    loop(0, lines, final_turn)

    def far_turn(k):
        keys = glob_ref[k].reshape(-1, head_size)
        held = glob_ref[kv_count + k].reshape(-1, head_size)
        for b in range(blocks_here):
            scores = scores_of(k, b, keys)
            far = []
            for s in range(ids_ref.shape[0]):
                gap = rank * blocks_here + b - ids_ref[s]
                shift = jnp.where((gap >= 0) & (gap < WIN), masked_score, 0.0)
                far.append(scores[:, s * BLK : (s + 1) * BLK] + shift)
            keep(k, b, absorb(k, b, jnp.concatenate(far, axis=1), held))

    loop(0, kv_count, far_turn)
    loop(1, lines, lambda j: along(j).wait_send())
    loop(1, n, lambda i: gather(i).wait_send())

    @pl.when(rank < n - 1)
    def _():
        near.wait_send()

    @pl.when(rank > 0)
    def _():
        near.wait_recv()

    def near_turn(k):
        for b in range(blocks_here):
            count = max(0, WIN - 1 - b)
            if count:
                keys = prev_ref[k, blocks_here - count :].reshape(count * BLK, head_size)
                held = prev_ref[kv_count + k, blocks_here - count :].reshape(count * BLK, head_size)
                scores = masked(scores_of(k, b, keys), bias_ref[b][:, : count * BLK])
                _, total, out = absorb(k, b, scores, held)
            else:
                total, out = total_ref[k, b], sum_ref[k, b]
            out = (out / total).astype(o_ref.dtype).reshape(group_size, BLK, head_size)
            o_ref[pl.ds(k * group_size, group_size), b * BLK : (b + 1) * BLK, :] = out

    loop(0, kv_count, near_turn)


def fused(ids, lens, q, own):
    n = lax.axis_size("seq")
    _, kv_count, tok_rows, head_size = own.shape
    sides = 2 * kv_count
    parts = n // sides
    part_rows = BLK // parts
    blocks_here = tok_rows // BLK
    rows = q.shape[0] // kv_count * BLK
    own = own.reshape(sides, blocks_here, parts, part_rows, head_size)
    smem = pl.BlockSpec(memory_space=pltpu.SMEM)
    vmem = pl.BlockSpec(memory_space=pltpu.VMEM)
    dma = pltpu.SemaphoreType.DMA
    return pl.pallas_call(
        functools.partial(fused_kernel, n),
        out_shape=jax.ShapeDtypeStruct(q.shape, q.dtype),
        in_specs=[smem, smem, vmem, vmem],
        out_specs=vmem,
        scratch_shapes=[
            pltpu.VMEM(own.shape, own.dtype),
            pltpu.VMEM((sides, ids.shape[0], parts, part_rows, head_size), own.dtype),
            pltpu.VMEM((n * blocks_here, part_rows, head_size), own.dtype),
            pltpu.VMEM((blocks_here, BLK, WIN * BLK), jnp.float32),
            pltpu.VMEM((kv_count, blocks_here, rows, 1), jnp.float32),
            pltpu.VMEM((kv_count, blocks_here, rows, 1), jnp.float32),
            pltpu.VMEM((kv_count, blocks_here, rows, head_size), jnp.float32),
            dma((n,)),
            dma((n,)),
            dma((n,)),
            dma((n,)),
            dma((2,)),
        ],
        compiler_params=pltpu.CompilerParams(collective_id=0, has_side_effects=True),
    )(ids, lens, q, own)


def per_device(queries, keys, values, global_ids, doc_lengths):
    own = jnp.stack([keys, values]).transpose(0, 2, 1, 3)
    q = queries.transpose(1, 0, 2)
    return fused(global_ids, doc_lengths, q, own).transpose(1, 0, 2)


def solution(mesh):
    tokens = P(("grp", "seq"), None, None)
    return jax.shard_map(
        per_device,
        mesh=mesh,
        in_specs=(tokens, tokens, tokens, P("grp"), P("grp")),
        out_specs=tokens,
        check_vma=False,
    )
```

```python
import functools
import math

import jax
import jax.numpy as jnp
from jax import lax
from jax.experimental import pallas as pl
from jax.experimental.pallas import tpu as pltpu
from jax.sharding import PartitionSpec as P

BLK = 128
WIN = 3

masked_score = -1e30


def fill_bias(rank, lens_ref, bias_ref):
    blocks_here, _, span = bias_ref.shape
    for b in range(blocks_here):
        first = (rank * blocks_here + b) * BLK
        query_pos = first + lax.broadcasted_iota(jnp.int32, (BLK, span), 0)
        key_pos = first - (WIN - 1) * BLK + lax.broadcasted_iota(jnp.int32, (BLK, span), 1)

        def step(d, carry):
            end, lowest = carry
            end = end + lens_ref[d]
            return end, jnp.where(query_pos >= end, end, lowest)

        _, lowest = lax.fori_loop(
            0, lens_ref.shape[0], step, (jnp.int32(0), jnp.zeros((BLK, span), jnp.int32))
        )
        seen = (key_pos >= lowest) & (key_pos <= query_pos)
        bias_ref[b] = jnp.where(seen, 0.0, masked_score)


def attn_kernel(ids_ref, lens_ref, q_ref, own_ref, prev_ref, glob_ref, o_ref, bias_ref):
    group_size, tok_rows, head_size = q_ref.shape
    blocks_here = tok_rows // BLK
    rank = lax.axis_index("seq")
    factor = math.log2(math.e) / math.sqrt(head_size)
    rows = group_size * BLK

    @pl.when(pl.program_id(0) == 0)
    def _():
        fill_bias(rank, lens_ref, bias_ref)

    def near(which, b):
        parts = []
        for i in range(blocks_here + b - WIN + 1, blocks_here + b + 1):
            src, j = (prev_ref, i) if i < blocks_here else (own_ref, i - blocks_here)
            parts.append(src[which, 0, j * BLK : (j + 1) * BLK, :])
        return jnp.concatenate(parts, axis=0)

    dims = (((1,), (1,)), ((), ()))
    for b in range(blocks_here):
        q = q_ref[:, b * BLK : (b + 1) * BLK, :].reshape(rows, head_size)
        s_near = lax.dot_general(q, near(0, b), dims, preferred_element_type=jnp.float32)
        s_near = (s_near.reshape(group_size, BLK, WIN * BLK) + bias_ref[b][None]).reshape(
            rows, WIN * BLK
        )
        s_far = lax.dot_general(q, glob_ref[0, 0], dims, preferred_element_type=jnp.float32)
        far = []
        for s in range(ids_ref.shape[0]):
            gap = rank * blocks_here + b - ids_ref[s]
            shift = jnp.where((gap >= 0) & (gap < WIN), masked_score, 0.0)
            far.append(s_far[:, s * BLK : (s + 1) * BLK] + shift)
        scores = jnp.concatenate([s_near] + far, axis=1)
        peak = jnp.max(scores, axis=1, keepdims=True)
        terms = jnp.exp2((scores - peak) * factor)
        weights = terms.astype(jnp.bfloat16)
        held = jnp.concatenate([near(1, b), glob_ref[1, 0]], axis=0)
        held = jnp.concatenate([held, jnp.ones_like(held)], axis=1)
        both = jnp.dot(weights, held, preferred_element_type=jnp.float32)
        out = both[:, :head_size] / both[:, head_size:]
        o_ref[:, b * BLK : (b + 1) * BLK, :] = out.astype(o_ref.dtype).reshape(
            group_size, BLK, head_size
        )


def attention(ids, lens, q, own, prev, glob):
    heads_here, tok_rows, head_size = q.shape
    kv_count = own.shape[1]
    group_size = heads_here // kv_count
    blocks_here = tok_rows // BLK
    smem = pl.BlockSpec(memory_space=pltpu.SMEM)
    q_spec = pl.BlockSpec((group_size, tok_rows, head_size), lambda k: (k, 0, 0))
    keyed = lambda n: pl.BlockSpec((2, 1, n, head_size), lambda k: (0, k, 0, 0))
    return pl.pallas_call(
        attn_kernel,
        grid=(kv_count,),
        out_shape=jax.ShapeDtypeStruct(q.shape, jnp.bfloat16),
        in_specs=[smem, smem, q_spec, keyed(tok_rows), keyed(tok_rows), keyed(glob.shape[2])],
        out_specs=q_spec,
        scratch_shapes=[pltpu.VMEM((blocks_here, BLK, WIN * BLK), jnp.float32)],
    )(ids, lens, q, own, prev, glob)


def exchange_kernel(n, ids_ref, own_ref, prev_ref, glob_ref, raw_ref, to_sem, from_sem, pass_sem, land_sem, near_sem):
    rank = lax.axis_index("seq")
    blocks_here, parts = own_ref.shape[1], own_ref.shape[2]
    lines = n // 4
    line, low = rank // 4, rank % 4
    pair = line * 4 + (low + 2) % 4
    partner = rank + 1 - 2 * (rank % 2)

    barrier = pltpu.get_barrier_semaphore()

    def greet(i, carry):
        pl.semaphore_signal(
            barrier, inc=1, device_id={"seq": (rank + i) % n}, device_id_type=pl.DeviceIdType.MESH
        )
        return carry

    lax.fori_loop(1, n, greet, 0)
    pl.semaphore_wait(barrier, n - 1)

    def remote(src, dst, send, recv, device):
        return pltpu.make_async_remote_copy(
            src_ref=src,
            dst_ref=dst,
            send_sem=send,
            recv_sem=recv,
            device_id={"seq": device},
            device_id_type=pl.DeviceIdType.MESH,
        )

    def gather(i):
        dest = (rank + i) % n
        return remote(
            own_ref.at[dest // parts, :, dest % parts],
            raw_ref.at[pl.ds(rank * blocks_here, blocks_here)],
            to_sem.at[i],
            from_sem.at[i],
            dest,
        )

    def spread(i, piece, device):
        region = glob_ref.at[piece // parts, :, piece % parts]
        return remote(region, region, pass_sem.at[i], land_sem.at[i], device)

    def loop(low_end, high_end, body):
        def step(i, carry):
            body(i)
            return carry

        lax.fori_loop(low_end, high_end, step, 0)

    near = remote(own_ref, prev_ref, near_sem.at[0], near_sem.at[1], (rank + 1) % n)
    loop(1, n, lambda i: gather(i).start())

    @pl.when(rank < n - 1)
    def _():
        near.start()

    @pl.when(rank == 0)
    def _():
        prev_ref[...] = jnp.zeros_like(prev_ref)

    raw_ref[pl.ds(rank * blocks_here, blocks_here)] = own_ref[rank // parts, :, rank % parts]
    loop(1, n, lambda i: gather(i).wait_recv())
    for s in range(ids_ref.shape[0]):
        glob_ref[rank // parts, s, rank % parts] = raw_ref[ids_ref[s]]

    mine = lambda j: ((line - j + lines) % lines) * 4 + low
    theirs = lambda j: ((line - j + lines) % lines) * 4 + (low + 2) % 4
    ahead = lambda j: ((line + j) % lines) * 4 + low
    along = lambda j: spread(j, rank, ahead(j))
    across = lambda j: spread(lines + j, mine(j), pair)
    over = lambda j: spread(2 * lines + j, mine(j), partner)
    last = lambda j: spread(3 * lines + j, theirs(j), partner)

    loop(1, lines, lambda j: along(j).start())

    def first_turn(j):
        @pl.when(j > 0)
        def _():
            along(j).wait_recv()

        across(j).start()
        over(j).start()

    loop(0, lines, first_turn)

    def second_turn(j):
        across(j).wait_recv()
        last(j).start()

    loop(0, lines, second_turn)

    def final_turn(j):
        over(j).wait_recv()
        last(j).wait_recv()
        across(j).wait_send()
        over(j).wait_send()
        last(j).wait_send()

    loop(0, lines, final_turn)
    loop(1, lines, lambda j: along(j).wait_send())
    loop(1, n, lambda i: gather(i).wait_send())

    @pl.when(rank < n - 1)
    def _():
        near.wait_send()

    @pl.when(rank > 0)
    def _():
        near.wait_recv()


def exchange(ids, own):
    n = lax.axis_size("seq")
    _, kv_count, tok_rows, head_size = own.shape
    sides = 2 * kv_count
    parts = n // sides
    part_rows = BLK // parts
    blocks_here = tok_rows // BLK
    own = own.reshape(sides, blocks_here, parts, part_rows, head_size)
    slots = ids.shape[0]
    vmem = pl.BlockSpec(memory_space=pltpu.VMEM)
    dma = pltpu.SemaphoreType.DMA
    prev, glob = pl.pallas_call(
        functools.partial(exchange_kernel, n),
        out_shape=(
            jax.ShapeDtypeStruct(own.shape, own.dtype),
            jax.ShapeDtypeStruct((sides, slots, parts, part_rows, head_size), own.dtype),
        ),
        in_specs=[pl.BlockSpec(memory_space=pltpu.SMEM), vmem],
        out_specs=(vmem, vmem),
        scratch_shapes=[
            pltpu.VMEM((n * blocks_here, part_rows, head_size), own.dtype),
            dma((n,)),
            dma((n,)),
            dma((n,)),
            dma((n,)),
            dma((2,)),
        ],
        compiler_params=pltpu.CompilerParams(collective_id=0, has_side_effects=True),
    )(ids, own)
    return (
        prev.reshape(2, kv_count, tok_rows, head_size),
        glob.reshape(2, kv_count, slots * BLK, head_size),
    )


def per_device(queries, keys, values, global_ids, doc_lengths):
    own = jnp.stack([keys, values]).transpose(0, 2, 1, 3)
    prev, glob = exchange(global_ids, own)
    q = queries.transpose(1, 0, 2)
    out = attention(global_ids, doc_lengths, q, own, prev, glob)
    return out.transpose(1, 0, 2)


def solution(mesh):
    tokens = P(("grp", "seq"), None, None)
    return jax.shard_map(
        per_device,
        mesh=mesh,
        in_specs=(tokens, tokens, tokens, P("grp"), P("grp")),
        out_specs=tokens,
        check_vma=False,
    )
```
